32 devices in a mesh: lon: 8 (over y, x, core), lat: 4 (over z).
Axes of the slice: x: 2, y: 2, z: 4, core: 2. Of those that a mesh axis runs over, the one named last changes fastest.
Arguments:
- normed: bfloat16 [8, 96, 192, 192], P(None, 'lat', 'lon'), may hold values from -6 to 6
- cotangent: bfloat16 [8, 96, 192, 192], P(None, 'lat', 'lon'), may hold values from -6 to 6
- weight_qkv: bfloat16 [192, 576], replicated, may hold values from -0.4375 to 0.4375
- weight_proj: bfloat16 [192, 192], replicated, may hold values from -0.4375 to 0.4375
- bias_table: bfloat16 [64, 6, 20736], P('lat'), may hold values from -6 to 390
Outputs:
- input_grad: bfloat16 [8, 96, 192, 192], P(None, 'lat', 'lon')
- qkv_grad: float32 [192, 576], replicated
- proj_grad: float32 [192, 192], replicated
- bias_grad: float32 [64, 6, 20736], P('lat')
The draws below stay inside these ranges and needn't reach their ends.
All inputs are finite; a program needn't handle non-finite values.
Results may differ from the reference program's by a relative error of at most 0.019.
Values may be sent and summed in bfloat16 or wider, within the bound.
A program may use at most 192 MiB of HBM per device.

```python
import jax
import jax.numpy as jnp
from jax import lax

C = 192
HEADS = 6
WIN_Z = 2
WIN_LAT = 6
WIN_LON = 12
WTOK = 144
NZ = 8
TYPES = 64
NLAT = 96
NLON = 192


def draw_bias_table(key, part):
    keys_list = jax.random.split(jax.random.fold_in(key, 17), 1)
    shape = (TYPES, HEADS, WTOK, WTOK)
    baseline = jnp.clip(jax.random.normal(keys_list[0], shape, jnp.float32), -6.0, 6.0)
    return baseline.reshape(TYPES, HEADS, WTOK * WTOK).astype(jnp.bfloat16)


def block_levels(stream_key, shape, shards, least, largest):
    factor_of, own = 1.0, jax.random.fold_in(stream_key, 6)
    for position, blocks in shards:
        heights = jnp.exp(jax.random.uniform(jax.random.fold_in(own, position), (blocks,), jnp.float32, least / len(shards), largest / len(shards)))
        factor_of = factor_of * jnp.repeat(heights, shape[position] // blocks).reshape([-1 if axis == position else 1 for axis in range(len(shape))])
    return factor_of


def gaussian(rng, dims, width, most, cuts=(), kind=jnp.bfloat16):
    level = block_levels(rng, dims, cuts, -0.22, 0.18) if cuts else 1.0
    entries = jax.random.normal(rng, dims, jnp.float32) * width * level
    return jnp.minimum(jnp.maximum(entries, -most), most).astype(kind)


def setup_inputs(seed: int = 0) -> dict:
    keys = jax.random.split(jax.random.key(seed), 6)
    return {
        "normed": gaussian(keys[0], (NZ, NLAT, NLON, C), 1.0, 6.0, ((1, 4), (2, 8))),
        "cotangent": gaussian(keys[1], (NZ, NLAT, NLON, C), 1.0, 6.0, ((1, 4), (2, 8))),
        "weight_qkv": gaussian(keys[2], (C, 3 * C), C ** -0.5, 0.4375),
        "weight_proj": gaussian(keys[3], (C, C), C ** -0.5, 0.4375),
        "bias_table": draw_bias_table(jax.random.fold_in(keys[5], 71), 0),
    }


def window_split(grid_field):
    levels, height, breadth = grid_field.shape[:3]
    trailing_dims = grid_field.shape[3:]
    shaped = grid_field.reshape((levels // WIN_Z, WIN_Z, height // WIN_LAT, WIN_LAT, breadth // WIN_LON, WIN_LON) + trailing_dims)
    axes_order = (0, 2, 4, 1, 3, 5) + tuple(range(6, 6 + len(trailing_dims)))
    return shaped.transpose(axes_order).reshape((-1, WTOK) + trailing_dims)


def window_merge(windowed, levels, height, breadth):
    channels = windowed.shape[-1]
    shaped = windowed.reshape(levels // WIN_Z, height // WIN_LAT, breadth // WIN_LON, WIN_Z, WIN_LAT, WIN_LON, channels)
    return shaped.transpose(0, 3, 1, 4, 2, 5, 6).reshape(levels, height, breadth, channels)


def window_backward(block_in, block_cot, block_region, block_live, block_types, bias_rows, weight_qkv, weight_proj):
    windows = block_in.shape[0]
    channels = block_in.shape[2]
    head_dim = channels // HEADS
    softmax_scale = head_dim ** -0.5
    high = lax.Precision.HIGHEST
    f32 = jnp.float32
    projected = jnp.einsum('bnc,cf->bnf', block_in.astype(f32), weight_qkv.astype(f32), precision=high).astype(jnp.bfloat16)
    projected = projected.reshape(windows, WTOK, 3, HEADS, head_dim)
    queries = projected[:, :, 0]
    key_rows = projected[:, :, 1]
    values = projected[:, :, 2]
    bias_add = jnp.dot(block_types, bias_rows.astype(f32), precision=high).reshape(windows, HEADS, WTOK, WTOK)
    scores = jnp.einsum('bqhd,bkhd->bhqk', queries.astype(f32), key_rows.astype(f32), precision=high) * softmax_scale + bias_add
    allowed = (block_region[:, :, None] == block_region[:, None, :]) & (block_live[:, :, None] == block_live[:, None, :])
    allowed = allowed[:, None]
    peak_score = jnp.max(jnp.where(allowed, scores, -1e30), axis=-1, keepdims=True)
    exp_terms = jnp.where(allowed, jnp.exp(scores - peak_score), 0.0)
    attn_probs = exp_terms / jnp.sum(exp_terms, axis=-1, keepdims=True)
    probs_b = attn_probs.astype(jnp.bfloat16)
    mixed = jnp.einsum('bhqk,bkhd->bqhd', probs_b.astype(f32), values.astype(f32), precision=high).astype(jnp.bfloat16)
    mixed = mixed.reshape(windows, WTOK, channels)
    grad_proj = jnp.einsum('bnc,bnf->cf', mixed.astype(f32), block_cot.astype(f32), precision=high)
    mixed_grad = jnp.einsum('bnf,cf->bnc', block_cot.astype(f32), weight_proj.astype(f32), precision=high).astype(jnp.bfloat16)
    mixed_grad = mixed_grad.reshape(windows, WTOK, HEADS, head_dim)
    prob_grad = jnp.einsum('bqhd,bkhd->bhqk', mixed_grad.astype(f32), values.astype(f32), precision=high)
    row_delta = jnp.sum(attn_probs * prob_grad, axis=-1, keepdims=True)
    score_grad = attn_probs * (prob_grad - row_delta)
    grad_bias = jnp.dot(block_types.T, score_grad.reshape(windows, -1), precision=high)
    score_grad_b = score_grad.astype(jnp.bfloat16).astype(f32)
    query_grad = (jnp.einsum('bhqk,bkhd->bqhd', score_grad_b, key_rows.astype(f32), precision=high) * softmax_scale).astype(jnp.bfloat16)
    key_grad = (jnp.einsum('bhqk,bqhd->bkhd', score_grad_b, queries.astype(f32), precision=high) * softmax_scale).astype(jnp.bfloat16)
    value_grad = jnp.einsum('bhqk,bqhd->bkhd', probs_b.astype(f32), mixed_grad.astype(f32), precision=high).astype(jnp.bfloat16)
    cols_grad = jnp.stack([query_grad, key_grad, value_grad], axis=2).reshape(windows, WTOK, 3 * channels)
    grad_qkv = jnp.einsum('bnc,bnf->cf', block_in.astype(f32), cols_grad.astype(f32), precision=high)
    grad_in = jnp.einsum('bnf,cf->bnc', cols_grad.astype(f32), weight_qkv.astype(f32), precision=high).astype(jnp.bfloat16)
    return grad_in, grad_qkv, grad_proj, grad_bias


def reference(normed, cotangent, weight_qkv, weight_proj, bias_table):
    levels, height, breadth, channels = normed.shape
    level_shift = WIN_Z // 2
    lat_shift = WIN_LAT // 2
    lon_shift = WIN_LON // 2

    def to_frame(grid_field):
        rolled = jnp.roll(jnp.roll(grid_field, -lon_shift, axis=2), -level_shift, axis=0)
        padding = jnp.zeros((levels, lat_shift, breadth, channels), grid_field.dtype)
        return jnp.concatenate([rolled[:, lat_shift:], padding], axis=1)

    framed_in = window_split(to_frame(normed))
    framed_cot = window_split(to_frame(cotangent))
    level_index = jnp.arange(levels, dtype=jnp.int32)
    wrapped_levels = (level_index >= levels - level_shift).astype(jnp.int32)
    wrapped_field = jnp.broadcast_to(wrapped_levels[:, None, None], (levels, height, breadth))
    region_win = window_split(wrapped_field)
    row_index = jnp.arange(height, dtype=jnp.int32)
    live_rows = row_index < height - lat_shift
    live_field = jnp.broadcast_to(live_rows[None, :, None], (levels, height, breadth))
    live_win = window_split(live_field)
    level_windows = levels // WIN_Z
    lat_windows = height // WIN_LAT
    lon_windows = breadth // WIN_LON
    level_part = jnp.arange(level_windows, dtype=jnp.int32)[:, None, None]
    lat_part = jnp.arange(lat_windows, dtype=jnp.int32)[None, :, None]
    kinds = jnp.broadcast_to(lat_part * level_windows + level_part, (level_windows, lat_windows, lon_windows))
    onehot = (kinds.reshape(-1)[:, None] == jnp.arange(TYPES, dtype=jnp.int32)[None, :]).astype(jnp.float32)
    bias_rows = bias_table.reshape(TYPES, -1)
    window_total = framed_in.shape[0]
    block_size = max(divisor for divisor in range(1, 65) if window_total % divisor == 0)
    blocks = window_total // block_size

    def regroup(array):
        return array.reshape((blocks, block_size) + array.shape[1:])

    def step_block(totals, pieces):
        grad_in, grad_qkv, grad_proj, grad_bias = window_backward(pieces[0], pieces[1], pieces[2], pieces[3], pieces[4], bias_rows, weight_qkv, weight_proj)
        return (totals[0] + grad_qkv, totals[1] + grad_proj, totals[2] + grad_bias), grad_in

    start = (jnp.zeros((channels, 3 * channels), jnp.float32), jnp.zeros((channels, channels), jnp.float32), jnp.zeros((TYPES, HEADS * WTOK * WTOK), jnp.float32))
    totals, grads = lax.scan(step_block, start, (regroup(framed_in), regroup(framed_cot), regroup(region_win), regroup(live_win), regroup(onehot)))
    framed_grad = window_merge(grads.reshape(window_total, WTOK, channels), levels, height, breadth)
    zeros_rows = jnp.zeros((levels, lat_shift, breadth, channels), jnp.bfloat16)
    unshifted = jnp.concatenate([zeros_rows, framed_grad[:, :height - lat_shift]], axis=1)
    input_grad = jnp.roll(jnp.roll(unshifted, lon_shift, axis=2), level_shift, axis=0)
    return input_grad, totals[0], totals[1], totals[2].reshape(TYPES, HEADS, WTOK * WTOK)
```

```python
import functools
import math

import jax
import jax.numpy as jnp
from jax import lax
from jax.experimental import pallas as pl
from jax.experimental.pallas import tpu as pltpu
from jax.sharding import PartitionSpec as P

HEADS = 6
WIN_Z = 2
WIN_LAT = 6
WIN_LON = 12
WTOK = 144
LANES = 128
TAIL = WTOK - LANES
HALO = 8
CHUNKS = 2
LOG2E = math.log2(math.e)
F32 = jnp.float32
BF16 = jnp.bfloat16


def ring_permute(block, axis, distance):
    size = lax.axis_size(axis)
    return lax.ppermute(block, axis, [((i - distance) % size, i) for i in range(size)])


def line_permute(block, axis, distance):
    size = lax.axis_size(axis)
    route = [(i - distance, i) for i in range(size) if 0 <= i - distance < size]
    return lax.ppermute(block, axis, route)


def mm(a, b, ca=1, cb=0):
    return lax.dot_general(a, b, (((ca,), (cb,)), ((), ())), preferred_element_type=F32)


def kernel(
    first_row,
    lat_windows,
    level_windows,
    lon_windows,
    last_ref,
    perm_ref,
    xa_ref,
    xb_ref,
    ca_ref,
    cb_ref,
    wqkv_ref,
    wproj_ref,
    bias_ref,
    gframe_ref,
    gqkv_ref,
    gproj_ref,
    gbias_ref,
    qm_s,
    mm_s,
    p_s,
    ds_s,
):
    step = pl.program_id(0)
    a = lax.rem(step, level_windows)
    b = step // level_windows + first_row
    channels = wqkv_ref.shape[0]
    head_dim = channels // HEADS
    scale = head_dim ** -0.5
    half = WIN_LAT * xa_ref.shape[2]

    @pl.when(step == 0)
    def _():
        gqkv_ref[...] = jnp.zeros_like(gqkv_ref)
        gproj_ref[...] = jnp.zeros_like(gproj_ref)

    perm = perm_ref[...]
    x_raw = jnp.concatenate(
        [xa_ref[...].reshape(half, channels), xb_ref[...].reshape(half, channels)], axis=0
    )
    c_raw = jnp.concatenate(
        [ca_ref[...].reshape(half, channels), cb_ref[...].reshape(half, channels)], axis=0
    )
    x = mm(perm, x_raw).astype(BF16)
    c = mm(perm, c_raw).astype(BF16)
    proj = mm(x, wqkv_ref[...]).astype(BF16)
    mgrad = mm(c, wproj_ref[...], 1, 1).astype(BF16)

    wrap_here = a == level_windows - 1
    dead_here = (b == lat_windows - 1) & (last_ref[0] == 1)
    per_level = WTOK // WIN_Z

    def classes(shape, dim):
        token = lax.broadcasted_iota(jnp.int32, shape, dim)
        upper = token >= per_level
        inner = jnp.where(upper, token - per_level, token)
        wrapped = jnp.where(upper & wrap_here, 2, 0)
        dead = jnp.where((inner >= per_level // 2) & dead_here, 1, 0)
        return wrapped + dead

    same = classes((WTOK, WTOK), 0) == classes((WTOK, WTOK), 1)
    mask_add = jnp.where(same, 0.0, -1e30)
    lane_head = lax.broadcasted_iota(jnp.int32, (1, channels), 1) // head_dim
    zero = jnp.zeros((), BF16)

    parts = []
    for w in range(lon_windows):
        rows = slice(w * WTOK, (w + 1) * WTOK)
        parts.append(
            (
                proj[rows, :channels],
                proj[rows, channels : 2 * channels],
                proj[rows, 2 * channels :],
                mgrad[rows],
            )
        )
    mixed = [jnp.zeros((WTOK, channels), F32) for _ in range(lon_windows)]
    dq = [jnp.zeros((WTOK, channels), F32) for _ in range(lon_windows)]
    for h in range(HEADS):
        hot = (lane_head == h).astype(BF16)
        hrows = slice(h * WTOK, (h + 1) * WTOK)
        shift = bias_ref[0, hrows, :].astype(F32) * LOG2E + mask_add
        gb = None
        for w in range(lon_windows):
            q, k, v, m = parts[w]
            qm = q * hot
            mg = m * hot
            qm_s[w, hrows, :] = qm
            mm_s[w, hrows, :] = mg
            s = mm(qm, k, 1, 1) * (scale * LOG2E) + shift
            dp = mm(mg, v, 1, 1)
            e = jnp.exp2(s - jnp.max(s, axis=1, keepdims=True))
            p = e * (1.0 / jnp.sum(e, axis=1, keepdims=True))
            delta = jnp.sum(p * dp, axis=1, keepdims=True)
            ds = p * (dp - delta)
            pb = p.astype(BF16)
            dsb = ds.astype(BF16)
            p_s[w, hrows, :] = pb
            ds_s[w, hrows, :] = dsb
            gb = ds if gb is None else gb + ds
            mixed[w] = mixed[w] + mm(pb, v * hot)
            dq[w] = dq[w] + mm(dsb, k * hot)
        gb = gb.astype(BF16)
        gbias_ref[0, hrows, :] = gb[:, :LANES]
        gbias_ref[0, HEADS * WTOK :, h * TAIL : (h + 1) * TAIL] = gb[:, LANES:]
    cols = []
    for w in range(lon_windows):
        dk = mm(ds_s[w], qm_s[w], 0, 0) * scale
        dv = mm(p_s[w], mm_s[w], 0, 0)
        cols.append(
            jnp.concatenate(
                [(dq[w] * scale).astype(BF16), dk.astype(BF16), dv.astype(BF16)], axis=1
            )
        )
    cols = jnp.concatenate(cols, axis=0)
    mixed_b = jnp.concatenate([t.astype(BF16) for t in mixed], axis=0)
    gproj_ref[...] += mm(mixed_b, c, 0, 0)
    gqkv_ref[...] += mm(x, cols, 0, 0)
    gin = mm(cols, wqkv_ref[...], 1, 1).astype(BF16)
    gout = mm(perm, gin, 0, 0).astype(BF16)
    gframe_ref[...] = gout.reshape(gframe_ref.shape)


def window_call(chunk, last, perm, frame_in, frame_cot, weight_qkv, weight_proj, bias):
    levels, height, wide, channels = frame_in.shape
    level_windows = levels // WIN_Z
    lat_windows = height // WIN_LAT
    lon_windows = perm.shape[0] // WTOK
    rows_here = lat_windows // CHUNKS
    first = chunk * rows_here
    kinds = rows_here * level_windows

    def at(step, up):
        z = lax.rem(WIN_Z * lax.rem(step, level_windows) + up, levels)
        return z, step // level_windows + first, 0, 0

    tok = (1, WIN_LAT, wide, channels)
    low = pl.BlockSpec(tok, lambda i: at(i, 1))
    high = pl.BlockSpec(tok, lambda i: at(i, 2))
    whole = lambda arr: pl.BlockSpec(arr.shape, lambda i: (0,) * arr.ndim)
    const = lambda shape: pl.BlockSpec(shape, lambda i: (0,) * len(shape))
    stack = HEADS * WTOK
    packed = stack + WTOK
    return pl.pallas_call(
        functools.partial(kernel, first, lat_windows, level_windows, lon_windows),
        grid=(kinds,),
        in_specs=[
            pl.BlockSpec(memory_space=pltpu.SMEM),
            whole(perm),
            low,
            high,
            low,
            high,
            whole(weight_qkv),
            whole(weight_proj),
            pl.BlockSpec((1, stack, WTOK), lambda i: (i + first * level_windows, 0, 0)),
        ],
        out_specs=[
            pl.BlockSpec(
                (WIN_Z, WIN_LAT, wide, channels),
                lambda i: (lax.rem(i, level_windows), i // level_windows, 0, 0),
            ),
            const((channels, 3 * channels)),
            const((channels, channels)),
            pl.BlockSpec((1, packed, LANES), lambda i: (i, 0, 0)),
        ],
        out_shape=[
            jax.ShapeDtypeStruct((levels, rows_here * WIN_LAT, wide, channels), BF16),
            jax.ShapeDtypeStruct((channels, 3 * channels), F32),
            jax.ShapeDtypeStruct((channels, channels), F32),
            jax.ShapeDtypeStruct((kinds, packed, LANES), BF16),
        ],
        scratch_shapes=[
            pltpu.VMEM((lon_windows, stack, channels), BF16),
            pltpu.VMEM((lon_windows, stack, channels), BF16),
            pltpu.VMEM((lon_windows, stack, WTOK), BF16),
            pltpu.VMEM((lon_windows, stack, WTOK), BF16),
        ],
        compiler_params=pltpu.CompilerParams(
            dimension_semantics=("arbitrary",), vmem_limit_bytes=48 * 2**20
        ),
        cost_estimate=pl.CostEstimate(
            flops=kinds * 1_500_000_000, bytes_accessed=kinds * 2_000_000, transcendentals=0
        ),
    )(
        last, perm, frame_in, frame_in, frame_cot, frame_cot, weight_qkv, weight_proj, bias
    )


def local(normed, cotangent, weight_qkv, weight_proj, bias_table):
    levels, height, breadth, channels = normed.shape
    lat_shift = WIN_LAT // 2
    lon_shift = WIN_LON // 2
    level_windows = levels // WIN_Z
    lat_windows = height // WIN_LAT
    lon_windows = breadth // WIN_LON
    types_local = level_windows * lat_windows
    wide = breadth + HALO
    across = ring_permute((normed[:, :, :HALO], cotangent[:, :, :HALO]), "lon", -1)
    wide_in = jnp.concatenate([normed, across[0]], axis=2)
    wide_cot = jnp.concatenate([cotangent, across[1]], axis=2)
    upward = line_permute((wide_in[:, :lat_shift], wide_cot[:, :lat_shift]), "lat", -1)
    frame_in = jnp.concatenate([wide_in[:, lat_shift:], upward[0]], axis=1)
    frame_cot = jnp.concatenate([wide_cot[:, lat_shift:], upward[1]], axis=1)
    last = (lax.axis_index("lat") == lax.axis_size("lat") - 1).astype(jnp.int32).reshape(1)
    bias = bias_table.reshape(types_local, HEADS * WTOK, WTOK)

    rows = jnp.arange(lon_windows * WTOK, dtype=jnp.int32)
    token = rows % WTOK
    per_level = WIN_LAT * WIN_LON
    source = (
        token // per_level * (WIN_LAT * wide)
        + token % per_level // WIN_LON * wide
        + rows // WTOK * WIN_LON
        + token % WIN_LON
        + lon_shift
    )
    columns = jnp.arange(WIN_Z * WIN_LAT * wide, dtype=jnp.int32)
    perm = (source[:, None] == columns[None, :]).astype(BF16)

    frames, qkv, proj, biases = [], 0.0, 0.0, []
    for chunk in range(CHUNKS):
        gframe, gqkv, gproj, gbias = window_call(
            chunk, last, perm, frame_in, frame_cot, weight_qkv, weight_proj, bias
        )
        frames.append(gframe)
        qkv = qkv + gqkv
        proj = proj + gproj
        biases.append(lax.psum(gbias, "lon"))

    gwide = jnp.roll(jnp.concatenate(frames, axis=1), WIN_Z // 2, axis=0)
    side = ring_permute(gwide[:, :, breadth:], "lon", 1)
    seam = jnp.concatenate(
        [gwide[:, :, :HALO] + side, gwide[:, :, HALO:breadth]], axis=2
    )
    down = line_permute(seam[:, height - lat_shift :], "lat", 1)
    input_grad = jnp.concatenate([down, seam[:, : height - lat_shift]], axis=1)
    qkv_grad, proj_grad = lax.psum((qkv.astype(BF16), proj.astype(BF16)), ("lat", "lon"))

    stack = HEADS * WTOK
    outs = []
    for packed in biases:
        kinds = packed.shape[0]
        head = packed[:, :stack].reshape(kinds, HEADS, WTOK, LANES)
        tail = packed[:, stack:, : HEADS * TAIL].reshape(kinds, WTOK, HEADS, TAIL)
        both = jnp.concatenate([head, tail.transpose(0, 2, 1, 3)], axis=3)
        outs.append(both.astype(F32).reshape(kinds, HEADS, WTOK * WTOK))
    bias_grad = jnp.concatenate(outs, axis=0)
    return input_grad, qkv_grad.astype(F32), proj_grad.astype(F32), bias_grad


def solution(mesh):
    in_specs = (
        P(None, "lat", "lon", None),
        P(None, "lat", "lon", None),
        P(),
        P(),
        P("lat", None, None),
    )
    out_specs = (P(None, "lat", "lon", None), P(), P(), P("lat", None, None))
    return jax.shard_map(local, mesh=mesh, in_specs=in_specs, out_specs=out_specs, check_vma=False)
```

```python
import functools
import math

import jax
import jax.numpy as jnp
from jax import lax
from jax.experimental import pallas as pl
from jax.experimental.pallas import tpu as pltpu
from jax.sharding import PartitionSpec as P

HEADS = 6
WIN_Z = 2
WIN_LAT = 6
WIN_LON = 12
WTOK = 144
LANES = 128
TAIL = WTOK - LANES
HALO = 8
CHUNKS = 1
LOG2E = math.log2(math.e)
F32 = jnp.float32
BF16 = jnp.bfloat16


def ring_permute(block, axis, distance):
    size = lax.axis_size(axis)
    return lax.ppermute(block, axis, [((i - distance) % size, i) for i in range(size)])


def line_permute(block, axis, distance):
    size = lax.axis_size(axis)
    route = [(i - distance, i) for i in range(size) if 0 <= i - distance < size]
    return lax.ppermute(block, axis, route)


def mm(a, b, ca=1, cb=0):
    return lax.dot_general(a, b, (((ca,), (cb,)), ((), ())), preferred_element_type=F32)


def kernel(
    first_row,
    lat_windows,
    level_windows,
    lon_windows,
    last_ref,
    perm_ref,
    xa_ref,
    xb_ref,
    ca_ref,
    cb_ref,
    wqkv_ref,
    wproj_ref,
    bias_ref,
    gframe_ref,
    gqkv_ref,
    gproj_ref,
    gbias_ref,
    qm_s,
    mm_s,
    p_s,
    ds_s,
):
    step = pl.program_id(0)
    a = lax.rem(step, level_windows)
    b = step // level_windows + first_row
    channels = wqkv_ref.shape[0]
    head_dim = channels // HEADS
    scale = head_dim ** -0.5
    half = WIN_LAT * xa_ref.shape[2]

    @pl.when(step == 0)
    def _():
        gqkv_ref[...] = jnp.zeros_like(gqkv_ref)
        gproj_ref[...] = jnp.zeros_like(gproj_ref)

    perm = perm_ref[...]
    x_raw = jnp.concatenate(
        [xa_ref[...].reshape(half, channels), xb_ref[...].reshape(half, channels)], axis=0
    )
    c_raw = jnp.concatenate(
        [ca_ref[...].reshape(half, channels), cb_ref[...].reshape(half, channels)], axis=0
    )
    x = mm(perm, x_raw).astype(BF16)
    c = mm(perm, c_raw).astype(BF16)
    proj = mm(x, wqkv_ref[...]).astype(BF16)
    mgrad = mm(c, wproj_ref[...], 1, 1).astype(BF16)

    wrap_here = a == level_windows - 1
    dead_here = (b == lat_windows - 1) & (last_ref[0] == 1)
    per_level = WTOK // WIN_Z

    def classes(shape, dim):
        token = lax.broadcasted_iota(jnp.int32, shape, dim)
        upper = token >= per_level
        inner = jnp.where(upper, token - per_level, token)
        wrapped = jnp.where(upper & wrap_here, 2, 0)
        dead = jnp.where((inner >= per_level // 2) & dead_here, 1, 0)
        return wrapped + dead

    same = classes((WTOK, WTOK), 0) == classes((WTOK, WTOK), 1)
    mask_add = jnp.where(same, 0.0, -1e30)
    lane_head = lax.broadcasted_iota(jnp.int32, (1, channels), 1) // head_dim
    zero = jnp.zeros((), BF16)

    parts = []
    for w in range(lon_windows):
        rows = slice(w * WTOK, (w + 1) * WTOK)
        parts.append(
            (
                proj[rows, :channels],
                proj[rows, channels : 2 * channels],
                proj[rows, 2 * channels :],
                mgrad[rows],
            )
        )
    mixed = [jnp.zeros((WTOK, channels), F32) for _ in range(lon_windows)]
    dq = [jnp.zeros((WTOK, channels), F32) for _ in range(lon_windows)]
    for h in range(HEADS):
        hot = (lane_head == h).astype(BF16)
        hrows = slice(h * WTOK, (h + 1) * WTOK)
        shift = bias_ref[0, hrows, :].astype(F32) * LOG2E + mask_add
        gb = None
        for w in range(lon_windows):
            q, k, v, m = parts[w]
            qm = q * hot
            mg = m * hot
            qm_s[w, hrows, :] = qm
            mm_s[w, hrows, :] = mg
            s = mm(qm, k, 1, 1) * (scale * LOG2E) + shift
            dp = mm(mg, v, 1, 1)
            e = jnp.exp2(s - jnp.max(s, axis=1, keepdims=True))
            p = e * (1.0 / jnp.sum(e, axis=1, keepdims=True))
            delta = jnp.sum(p * dp, axis=1, keepdims=True)
            ds = p * (dp - delta)
            pb = p.astype(BF16)
            dsb = ds.astype(BF16)
            p_s[w, hrows, :] = pb
            ds_s[w, hrows, :] = dsb
            gb = ds if gb is None else gb + ds
            mixed[w] = mixed[w] + mm(pb, v * hot)
            dq[w] = dq[w] + mm(dsb, k * hot)
        gb = gb.astype(BF16)
        gbias_ref[0, hrows, :] = gb[:, :LANES]
        gbias_ref[0, HEADS * WTOK :, h * TAIL : (h + 1) * TAIL] = gb[:, LANES:]
    cols = []
    for w in range(lon_windows):
        dk = mm(ds_s[w], qm_s[w], 0, 0) * scale
        dv = mm(p_s[w], mm_s[w], 0, 0)
        cols.append(
            jnp.concatenate(
                [(dq[w] * scale).astype(BF16), dk.astype(BF16), dv.astype(BF16)], axis=1
            )
        )
    cols = jnp.concatenate(cols, axis=0)
    mixed_b = jnp.concatenate([t.astype(BF16) for t in mixed], axis=0)
    gproj_ref[...] += mm(mixed_b, c, 0, 0)
    gqkv_ref[...] += mm(x, cols, 0, 0)
    gin = mm(cols, wqkv_ref[...], 1, 1).astype(BF16)
    gout = mm(perm, gin, 0, 0).astype(BF16)
    gframe_ref[...] = gout.reshape(gframe_ref.shape)


def reduce_kernel(
    n, lats, gb_ref, wg_ref, out_ref, wout_ref, pair_s, send_s, recv_s, w1_s, w2_s,
    pair_sem, cross_sem, back_sem, fwd_sem, w1_sem, w2_sem, w3_sem,
):
    chips = n // 2
    me = lax.axis_index("lon")
    lat = lax.axis_index("lat")
    core = lax.rem(me, 2)
    chip = me // 2
    other = 1 - core
    partner = chip * 2 + other
    types = gb_ref.shape[0]
    share = types // n

    def piece(which, where):
        return pl.ds((which * chips + where) * share, share)

    def copy(src, dst, sems, out_at, in_at, device):
        return pltpu.make_async_remote_copy(
            src_ref=src,
            dst_ref=dst,
            send_sem=sems.at[0, out_at],
            recv_sem=sems.at[1, in_at],
            device_id=device,
            device_id_type=pl.DeviceIdType.MESH,
        )

    barrier = pltpu.get_barrier_semaphore()
    for o in range(1, n):
        pl.semaphore_signal(
            barrier, inc=1, device_id={"lon": lax.rem(me + o, n)},
            device_id_type=pl.DeviceIdType.MESH,
        )
    for o in range(1, lats):
        pl.semaphore_signal(
            barrier, inc=1, device_id={"lat": lax.rem(lat + o, lats)},
            device_id_type=pl.DeviceIdType.MESH,
        )
    pl.semaphore_wait(barrier, n + lats - 2)

    order = [(o, lax.rem(chip + o, chips)) for o in list(range(1, chips)) + [0]]
    sends = []
    first = []
    for o in range(1, n):
        p = lax.rem(me + o, n)
        cp = copy(wg_ref.at[p], w1_s.at[me], w1_sem, p, me, {"lon": p})
        cp.start()
        sends.append(cp)
    for o, j in order:
        cp = copy(gb_ref.at[piece(other, j)], pair_s.at[o], pair_sem, o, o, {"lon": partner})
        cp.start()
        first.append(cp)
    sends += first

    w1_s[pl.ds(me, 1)] = wg_ref[pl.ds(me, 1)]
    for o in range(1, n):
        p = lax.rem(me + o, n)
        copy(wg_ref.at[p], w1_s.at[p], w1_sem, p, p, {"lon": p}).wait_recv()
    w2_s[pl.ds(lat, 1)] = jnp.sum(w1_s[...].astype(F32), axis=0, keepdims=True).astype(BF16)
    for o in range(1, lats):
        p = lax.rem(lat + o, lats)
        cp = copy(w2_s.at[lat], w2_s.at[lat], w2_sem, p, lat, {"lat": p})
        cp.start()
        sends.append(cp)

    for cp, (o, j) in zip(first, order):
        cp.wait_recv()

        def add(i, _, o=o, j=j):
            mine = gb_ref[(core * chips + j) * share + i].astype(F32)
            total = (mine + pair_s[o, i].astype(F32)).astype(BF16)
            if o:
                send_s[o, i] = total
            else:
                recv_s[chip, i] = total
            return 0

        lax.fori_loop(0, share, add, 0)
        if o:
            cp2 = copy(
                send_s.at[o], recv_s.at[chip], cross_sem, o, chip, {"lon": j * 2 + core}
            )
            cp2.start()
            sends.append(cp2)

    for o in range(1, lats):
        p = lax.rem(lat + o, lats)
        copy(w2_s.at[p], w2_s.at[p], w2_sem, p, p, {"lat": p}).wait_recv()
    wout_ref[pl.ds(me, 1)] = jnp.sum(w2_s[...].astype(F32), axis=0, keepdims=True).astype(BF16)
    for o in range(1, n):
        p = lax.rem(me + o, n)
        cp = copy(wout_ref.at[me], wout_ref.at[me], w3_sem, p, me, {"lon": p})
        cp.start()
        sends.append(cp)

    for o in range(1, chips):
        j = lax.rem(chip + o, chips)
        copy(send_s.at[o], recv_s.at[j], cross_sem, o, j, {"lon": j * 2 + core}).wait_recv()

    def total(i, _):
        acc = recv_s[0, i].astype(F32)
        for j in range(1, chips):
            acc = acc + recv_s[j, i].astype(F32)
        out_ref[(core * chips + chip) * share + i] = acc.astype(BF16)
        return 0

    lax.fori_loop(0, share, total, 0)
    own = out_ref.at[piece(core, chip)]
    for o in range(1, chips):
        j = lax.rem(chip + o, chips)
        cp = copy(own, own, back_sem, j, chip, {"lon": j * 2 + core})
        cp.start()
        sends.append(cp)
    cp = copy(own, own, fwd_sem, chip, chip, {"lon": partner})
    cp.start()
    sends.append(cp)
    for o in range(1, chips):
        j = lax.rem(chip + o, chips)
        part = out_ref.at[piece(core, j)]
        copy(part, part, back_sem, j, j, {"lon": j * 2 + core}).wait_recv()
        cp = copy(part, part, fwd_sem, j, j, {"lon": partner})
        cp.start()
        sends.append(cp)
    for j in range(chips):
        part = out_ref.at[piece(other, j)]
        copy(part, part, fwd_sem, j, j, {"lon": partner}).wait_recv()
    for o in range(1, n):
        p = lax.rem(me + o, n)
        copy(wout_ref.at[p], wout_ref.at[p], w3_sem, p, p, {"lon": p}).wait_recv()
    for cp in sends:
        cp.wait_send()


def reduce_all(gbias, weights):
    n, lats = lax.axis_size("lon"), lax.axis_size("lat")
    chips = n // 2
    types, packed, lanes = gbias.shape
    rows, width = weights.shape
    share = types // n
    weights = weights.reshape(n, rows // n, width)
    vm = pl.BlockSpec(memory_space=pltpu.VMEM)
    sem = lambda k: pltpu.SemaphoreType.DMA((2, k))
    block = pltpu.VMEM((chips, share, packed, lanes), BF16)
    out, wout = pl.pallas_call(
        functools.partial(reduce_kernel, n, lats),
        in_specs=[vm, vm],
        out_specs=[vm, vm],
        out_shape=[
            jax.ShapeDtypeStruct(gbias.shape, BF16),
            jax.ShapeDtypeStruct(weights.shape, BF16),
        ],
        scratch_shapes=[
            block,
            block,
            block,
            pltpu.VMEM((n, rows // n, width), BF16),
            pltpu.VMEM((lats, rows // n, width), BF16),
            sem(chips),
            sem(chips),
            sem(chips),
            sem(chips),
            sem(n),
            sem(lats),
            sem(n),
        ],
        compiler_params=pltpu.CompilerParams(
            collective_id=0, has_side_effects=True, vmem_limit_bytes=40 * 2**20
        ),
        cost_estimate=pl.CostEstimate(
            flops=30_000_000_000, bytes_accessed=60_000_000, transcendentals=0
        ),
    )(gbias, weights)
    return out, wout.reshape(rows, width)


def window_call(chunk, last, perm, frame_in, frame_cot, weight_qkv, weight_proj, bias):
    levels, height, wide, channels = frame_in.shape
    level_windows = levels // WIN_Z
    lat_windows = height // WIN_LAT
    lon_windows = perm.shape[0] // WTOK
    rows_here = lat_windows // CHUNKS
    first = chunk * rows_here
    kinds = rows_here * level_windows

    def at(step, up):
        z = lax.rem(WIN_Z * lax.rem(step, level_windows) + up, levels)
        return z, step // level_windows + first, 0, 0

    tok = (1, WIN_LAT, wide, channels)
    low = pl.BlockSpec(tok, lambda i: at(i, 1))
    high = pl.BlockSpec(tok, lambda i: at(i, 2))
    whole = lambda arr: pl.BlockSpec(arr.shape, lambda i: (0,) * arr.ndim)
    const = lambda shape: pl.BlockSpec(shape, lambda i: (0,) * len(shape))
    stack = HEADS * WTOK
    packed = stack + WTOK
    return pl.pallas_call(
        functools.partial(kernel, first, lat_windows, level_windows, lon_windows),
        grid=(kinds,),
        in_specs=[
            pl.BlockSpec(memory_space=pltpu.SMEM),
            whole(perm),
            low,
            high,
            low,
            high,
            whole(weight_qkv),
            whole(weight_proj),
            pl.BlockSpec((1, stack, WTOK), lambda i: (i + first * level_windows, 0, 0)),
        ],
        out_specs=[
            pl.BlockSpec(
                (WIN_Z, WIN_LAT, wide, channels),
                lambda i: (lax.rem(i, level_windows), i // level_windows, 0, 0),
            ),
            const((channels, 3 * channels)),
            const((channels, channels)),
            pl.BlockSpec((1, packed, LANES), lambda i: (i, 0, 0)),
        ],
        out_shape=[
            jax.ShapeDtypeStruct((levels, rows_here * WIN_LAT, wide, channels), BF16),
            jax.ShapeDtypeStruct((channels, 3 * channels), F32),
            jax.ShapeDtypeStruct((channels, channels), F32),
            jax.ShapeDtypeStruct((kinds, packed, LANES), BF16),
        ],
        scratch_shapes=[
            pltpu.VMEM((lon_windows, stack, channels), BF16),
            pltpu.VMEM((lon_windows, stack, channels), BF16),
            pltpu.VMEM((lon_windows, stack, WTOK), BF16),
            pltpu.VMEM((lon_windows, stack, WTOK), BF16),
        ],
        compiler_params=pltpu.CompilerParams(
            dimension_semantics=("arbitrary",), vmem_limit_bytes=48 * 2**20
        ),
        cost_estimate=pl.CostEstimate(
            flops=kinds * 1_500_000_000, bytes_accessed=kinds * 2_000_000, transcendentals=0
        ),
    )(
        last, perm, frame_in, frame_in, frame_cot, frame_cot, weight_qkv, weight_proj, bias
    )


def local(normed, cotangent, weight_qkv, weight_proj, bias_table):
    levels, height, breadth, channels = normed.shape
    lat_shift = WIN_LAT // 2
    lon_shift = WIN_LON // 2
    level_windows = levels // WIN_Z
    lat_windows = height // WIN_LAT
    lon_windows = breadth // WIN_LON
    types_local = level_windows * lat_windows
    wide = breadth + HALO
    across = ring_permute((normed[:, :, :HALO], cotangent[:, :, :HALO]), "lon", -1)
    wide_in = jnp.concatenate([normed, across[0]], axis=2)
    wide_cot = jnp.concatenate([cotangent, across[1]], axis=2)
    upward = line_permute((wide_in[:, :lat_shift], wide_cot[:, :lat_shift]), "lat", -1)
    frame_in = jnp.concatenate([wide_in[:, lat_shift:], upward[0]], axis=1)
    frame_cot = jnp.concatenate([wide_cot[:, lat_shift:], upward[1]], axis=1)
    last = (lax.axis_index("lat") == lax.axis_size("lat") - 1).astype(jnp.int32).reshape(1)
    bias = bias_table.reshape(types_local, HEADS * WTOK, WTOK)

    rows = jnp.arange(lon_windows * WTOK, dtype=jnp.int32)
    token = rows % WTOK
    per_level = WIN_LAT * WIN_LON
    source = (
        token // per_level * (WIN_LAT * wide)
        + token % per_level // WIN_LON * wide
        + rows // WTOK * WIN_LON
        + token % WIN_LON
        + lon_shift
    )
    columns = jnp.arange(WIN_Z * WIN_LAT * wide, dtype=jnp.int32)
    perm = (source[:, None] == columns[None, :]).astype(BF16)

    gframe, gqkv, gproj, gbias = window_call(
        0, last, perm, frame_in, frame_cot, weight_qkv, weight_proj, bias
    )
    weights = jnp.concatenate([gqkv, gproj], axis=1).astype(BF16)
    packed, weights = reduce_all(gbias, weights)
    weights = weights.astype(F32)

    gwide = jnp.roll(gframe, WIN_Z // 2, axis=0)
    side = ring_permute(gwide[:, :, breadth:], "lon", 1)
    seam = jnp.concatenate(
        [gwide[:, :, :HALO] + side, gwide[:, :, HALO:breadth]], axis=2
    )
    down = line_permute(seam[:, height - lat_shift :], "lat", 1)
    input_grad = jnp.concatenate([down, seam[:, : height - lat_shift]], axis=1)

    stack = HEADS * WTOK
    kinds = packed.shape[0]
    head = packed[:, :stack].reshape(kinds, HEADS, WTOK, LANES)
    tail = packed[:, stack:, : HEADS * TAIL].reshape(kinds, WTOK, HEADS, TAIL)
    both = jnp.concatenate([head, tail.transpose(0, 2, 1, 3)], axis=3)
    bias_grad = both.astype(F32).reshape(kinds, HEADS, WTOK * WTOK)
    return input_grad, weights[:, : 3 * channels], weights[:, 3 * channels :], bias_grad


def solution(mesh):
    in_specs = (
        P(None, "lat", "lon", None),
        P(None, "lat", "lon", None),
        P(),
        P(),
        P("lat", None, None),
    )
    out_specs = (P(None, "lat", "lon", None), P(), P(), P("lat", None, None))
    return jax.shard_map(local, mesh=mesh, in_specs=in_specs, out_specs=out_specs, check_vma=False)
```

```python
import functools
import math

import jax
import jax.numpy as jnp
from jax import lax
from jax.experimental import pallas as pl
from jax.experimental.pallas import tpu as pltpu
from jax.sharding import PartitionSpec as P

HEADS = 6
WIN_Z = 2
WIN_LAT = 6
WIN_LON = 12
WTOK = 144
LANES = 128
TAIL = WTOK - LANES
HALO = 8
CHUNKS = 1
LOG2E = math.log2(math.e)
F32 = jnp.float32
BF16 = jnp.bfloat16


def ring_permute(block, axis, distance):
    size = lax.axis_size(axis)
    return lax.ppermute(block, axis, [((i - distance) % size, i) for i in range(size)])


def line_permute(block, axis, distance):
    size = lax.axis_size(axis)
    route = [(i - distance, i) for i in range(size) if 0 <= i - distance < size]
    return lax.ppermute(block, axis, route)


def mm(a, b, ca=1, cb=0):
    return lax.dot_general(a, b, (((ca,), (cb,)), ((), ())), preferred_element_type=F32)


def kernel(
    first_row,
    lat_windows,
    level_windows,
    lon_windows,
    last_ref,
    perm_ref,
    xa_ref,
    xb_ref,
    ca_ref,
    cb_ref,
    wqkv_ref,
    wproj_ref,
    bias_ref,
    gframe_ref,
    gqkv_ref,
    gproj_ref,
    gbias_ref,
    qm_s,
    mm_s,
    p_s,
    ds_s,
):
    step = pl.program_id(0)
    a = lax.rem(step, level_windows)
    b = step // level_windows + first_row
    channels = wqkv_ref.shape[0]
    head_dim = channels // HEADS
    scale = head_dim ** -0.5
    half = WIN_LAT * xa_ref.shape[2]

    @pl.when(step == 0)
    def _():
        gqkv_ref[...] = jnp.zeros_like(gqkv_ref)
        gproj_ref[...] = jnp.zeros_like(gproj_ref)

    perm = perm_ref[...]
    x_raw = jnp.concatenate(
        [xa_ref[...].reshape(half, channels), xb_ref[...].reshape(half, channels)], axis=0
    )
    c_raw = jnp.concatenate(
        [ca_ref[...].reshape(half, channels), cb_ref[...].reshape(half, channels)], axis=0
    )
    x = mm(perm, x_raw).astype(BF16)
    c = mm(perm, c_raw).astype(BF16)
    proj = mm(x, wqkv_ref[...]).astype(BF16)
    mgrad = mm(c, wproj_ref[...], 1, 1).astype(BF16)

    wrap_here = a == level_windows - 1
    dead_here = (b == lat_windows - 1) & (last_ref[0] == 1)
    per_level = WTOK // WIN_Z

    def classes(shape, dim):
        token = lax.broadcasted_iota(jnp.int32, shape, dim)
        upper = token >= per_level
        inner = jnp.where(upper, token - per_level, token)
        wrapped = jnp.where(upper & wrap_here, 2, 0)
        dead = jnp.where((inner >= per_level // 2) & dead_here, 1, 0)
        return wrapped + dead

    same = classes((WTOK, WTOK), 0) == classes((WTOK, WTOK), 1)
    mask_add = jnp.where(same, 0.0, -1e30)
    lane_head = lax.broadcasted_iota(jnp.int32, (1, channels), 1) // head_dim
    zero = jnp.zeros((), BF16)

    parts = []
    for w in range(lon_windows):
        rows = slice(w * WTOK, (w + 1) * WTOK)
        parts.append(
            (
                proj[rows, :channels],
                proj[rows, channels : 2 * channels],
                proj[rows, 2 * channels :],
                mgrad[rows],
            )
        )
    mixed = [jnp.zeros((WTOK, channels), F32) for _ in range(lon_windows)]
    dq = [jnp.zeros((WTOK, channels), F32) for _ in range(lon_windows)]
    for h in range(HEADS):
        hot = (lane_head == h).astype(BF16)
        hrows = slice(h * WTOK, (h + 1) * WTOK)
        shift = bias_ref[0, hrows, :].astype(F32) * LOG2E + mask_add
        gb = None
        for w in range(lon_windows):
            q, k, v, m = parts[w]
            qm = q * hot
            mg = m * hot
            qm_s[w, hrows, :] = qm
            mm_s[w, hrows, :] = mg
            s = mm(qm, k, 1, 1) * (scale * LOG2E) + shift
            dp = mm(mg, v, 1, 1)
            e = jnp.exp2(s - jnp.max(s, axis=1, keepdims=True))
            p = e * (1.0 / jnp.sum(e, axis=1, keepdims=True))
            delta = jnp.sum(p * dp, axis=1, keepdims=True)
            ds = p * (dp - delta)
            pb = p.astype(BF16)
            dsb = ds.astype(BF16)
            p_s[w, hrows, :] = pb
            ds_s[w, hrows, :] = dsb
            gb = ds if gb is None else gb + ds
            mixed[w] = mixed[w] + mm(pb, v * hot)
            dq[w] = dq[w] + mm(dsb, k * hot)
        gb = gb.astype(BF16)
        gbias_ref[0, hrows, :] = gb[:, :LANES]
        gbias_ref[0, HEADS * WTOK :, h * TAIL : (h + 1) * TAIL] = gb[:, LANES:]
    cols = []
    for w in range(lon_windows):
        dk = mm(ds_s[w], qm_s[w], 0, 0) * scale
        dv = mm(p_s[w], mm_s[w], 0, 0)
        cols.append(
            jnp.concatenate(
                [(dq[w] * scale).astype(BF16), dk.astype(BF16), dv.astype(BF16)], axis=1
            )
        )
    cols = jnp.concatenate(cols, axis=0)
    mixed_b = jnp.concatenate([t.astype(BF16) for t in mixed], axis=0)
    gproj_ref[...] += mm(mixed_b, c, 0, 0)
    gqkv_ref[...] += mm(x, cols, 0, 0)
    gin = mm(cols, wqkv_ref[...], 1, 1).astype(BF16)
    gout = mm(perm, gin, 0, 0).astype(BF16)
    gframe_ref[...] = gout.reshape(gframe_ref.shape)


def reduce_kernel(
    n, lats, gb_ref, wg_ref, out_ref, wout_ref, pair_s, send_s, recv_s, w1_s, w2_s,
    pair_sem, cross_sem, back_sem, fwd_sem, w1_sem, w2_sem, w3_sem,
):
    chips = n // 2
    me = lax.axis_index("lon")
    lat = lax.axis_index("lat")
    core = lax.rem(me, 2)
    chip = me // 2
    other = 1 - core
    partner = chip * 2 + other
    types = gb_ref.shape[0]
    share = types // n

    def piece(which, where):
        return pl.ds((which * chips + where) * share, share)

    def copy(src, dst, sems, out_at, in_at, device):
        return pltpu.make_async_remote_copy(
            src_ref=src,
            dst_ref=dst,
            send_sem=sems.at[0, out_at],
            recv_sem=sems.at[1, in_at],
            device_id=device,
            device_id_type=pl.DeviceIdType.MESH,
        )

    barrier = pltpu.get_barrier_semaphore()
    for o in range(1, n):
        pl.semaphore_signal(
            barrier, inc=1, device_id={"lon": lax.rem(me + o, n)},
            device_id_type=pl.DeviceIdType.MESH,
        )
    for o in range(1, lats):
        pl.semaphore_signal(
            barrier, inc=1, device_id={"lat": lax.rem(lat + o, lats)},
            device_id_type=pl.DeviceIdType.MESH,
        )
    pl.semaphore_wait(barrier, n + lats - 2)

    order = [(o, lax.rem(chip + o, chips)) for o in list(range(1, chips)) + [0]]
    sends = []
    first = []
    for o in range(1, n):
        p = lax.rem(me + o, n)
        cp = copy(wg_ref.at[p], w1_s.at[me], w1_sem, p, me, {"lon": p})
        cp.start()
        sends.append(cp)
    for o, j in order:
        cp = copy(gb_ref.at[piece(other, j)], pair_s.at[o], pair_sem, o, o, {"lon": partner})
        cp.start()
        first.append(cp)
    sends += first

    w1_s[pl.ds(me, 1)] = wg_ref[pl.ds(me, 1)]
    for o in range(1, n):
        p = lax.rem(me + o, n)
        copy(wg_ref.at[p], w1_s.at[p], w1_sem, p, p, {"lon": p}).wait_recv()
    w2_s[pl.ds(lat, 1)] = jnp.sum(w1_s[...].astype(F32), axis=0, keepdims=True).astype(BF16)
    for o in range(1, lats):
        p = lax.rem(lat + o, lats)
        cp = copy(w2_s.at[lat], w2_s.at[lat], w2_sem, p, lat, {"lat": p})
        cp.start()
        sends.append(cp)

    for cp, (o, j) in zip(first, order):
        cp.wait_recv()

        def add(i, _, o=o, j=j):
            mine = gb_ref[(core * chips + j) * share + i].astype(F32)
            total = (mine + pair_s[o, i].astype(F32)).astype(BF16)
            if o:
                send_s[o, i] = total
            else:
                recv_s[chip, i] = total
            return 0

        lax.fori_loop(0, share, add, 0)
        if o:
            cp2 = copy(
                send_s.at[o], recv_s.at[chip], cross_sem, o, chip, {"lon": j * 2 + core}
            )
            cp2.start()
            sends.append(cp2)

    for o in range(1, lats):
        p = lax.rem(lat + o, lats)
        copy(w2_s.at[p], w2_s.at[p], w2_sem, p, p, {"lat": p}).wait_recv()
    wout_ref[pl.ds(me, 1)] = jnp.sum(w2_s[...].astype(F32), axis=0, keepdims=True).astype(BF16)
    for o in range(1, n):
        p = lax.rem(me + o, n)
        cp = copy(wout_ref.at[me], wout_ref.at[me], w3_sem, p, me, {"lon": p})
        cp.start()
        sends.append(cp)

    for o in range(1, chips):
        j = lax.rem(chip + o, chips)
        copy(send_s.at[o], recv_s.at[j], cross_sem, o, j, {"lon": j * 2 + core}).wait_recv()

    def total(i, _):
        acc = recv_s[0, i].astype(F32)
        for j in range(1, chips):
            acc = acc + recv_s[j, i].astype(F32)
        out_ref[(core * chips + chip) * share + i] = acc.astype(BF16)
        return 0

    lax.fori_loop(0, share, total, 0)
    own = out_ref.at[piece(core, chip)]
    for o in range(1, chips):
        j = lax.rem(chip + o, chips)
        cp = copy(own, own, back_sem, j, chip, {"lon": j * 2 + core})
        cp.start()
        sends.append(cp)
    cp = copy(own, own, fwd_sem, chip, chip, {"lon": partner})
    cp.start()
    sends.append(cp)
    for o in range(1, chips):
        j = lax.rem(chip + o, chips)
        part = out_ref.at[piece(core, j)]
        copy(part, part, back_sem, j, j, {"lon": j * 2 + core}).wait_recv()
        cp = copy(part, part, fwd_sem, j, j, {"lon": partner})
        cp.start()
        sends.append(cp)
    for j in range(chips):
        part = out_ref.at[piece(other, j)]
        copy(part, part, fwd_sem, j, j, {"lon": partner}).wait_recv()
    for o in range(1, n):
        p = lax.rem(me + o, n)
        copy(wout_ref.at[p], wout_ref.at[p], w3_sem, p, p, {"lon": p}).wait_recv()
    for cp in sends:
        cp.wait_send()


def reduce_all(gbias, weights):
    n, lats = lax.axis_size("lon"), lax.axis_size("lat")
    chips = n // 2
    types, packed, lanes = gbias.shape
    rows, width = weights.shape
    share = types // n
    weights = weights.reshape(n, rows // n, width)
    vm = pl.BlockSpec(memory_space=pltpu.VMEM)
    sem = lambda k: pltpu.SemaphoreType.DMA((2, k))
    block = pltpu.VMEM((chips, share, packed, lanes), BF16)
    out, wout = pl.pallas_call(
        functools.partial(reduce_kernel, n, lats),
        in_specs=[vm, vm],
        out_specs=[vm, vm],
        out_shape=[
            jax.ShapeDtypeStruct(gbias.shape, BF16),
            jax.ShapeDtypeStruct(weights.shape, BF16),
        ],
        scratch_shapes=[
            block,
            block,
            block,
            pltpu.VMEM((n, rows // n, width), BF16),
            pltpu.VMEM((lats, rows // n, width), BF16),
            sem(chips),
            sem(chips),
            sem(chips),
            sem(chips),
            sem(n),
            sem(lats),
            sem(n),
        ],
        compiler_params=pltpu.CompilerParams(
            collective_id=0, has_side_effects=True, vmem_limit_bytes=40 * 2**20
        ),
        cost_estimate=pl.CostEstimate(
            flops=30_000_000_000, bytes_accessed=60_000_000, transcendentals=0
        ),
    )(gbias, weights)
    return out, wout.reshape(rows, width)


def unpack_kernel(packed_ref, out_ref, main_s, tail_s):
    stack = HEADS * WTOK
    main_s[...] = packed_ref[0, :stack].astype(F32)
    tails = packed_ref[0, stack:].astype(F32)
    for h in range(HEADS):
        turned = tails if h == 0 else pltpu.roll(tails, LANES - h * TAIL, 1)
        tail_s[h * WTOK : (h + 1) * WTOK] = turned
    group = LANES // TAIL
    lane = lax.broadcasted_iota(jnp.int32, (HEADS, LANES), 1)

    def body(m, _):
        before_main = before_tail = None
        for r in range(group + 1):
            tile = None
            if r < group:
                at = pl.ds(m * group + r, HEADS, stride=WTOK)
                here_main, here_tail = main_s[at, :], tail_s[at, :]
                if r:
                    here_main = pltpu.roll(here_main, TAIL * r, 1)
                    here_tail = pltpu.roll(here_tail, TAIL * r, 1)
                tile = here_main
            if r:
                ended = before_tail
                if r > 1:
                    ended = jnp.where(lane < TAIL * (r - 1), before_main, before_tail)
                tile = ended if r == group else jnp.where(lane < TAIL * r, ended, tile)
            start = pl.multiple_of(m * (group * WTOK) + r * LANES, LANES)
            out_ref[0, :, pl.ds(start, LANES)] = tile
            if r < group:
                before_main, before_tail = here_main, here_tail
        return 0

    lax.fori_loop(0, WTOK // group, body, 0)


def unpack(packed):
    kinds, rows, lanes = packed.shape
    stack = HEADS * WTOK
    return pl.pallas_call(
        unpack_kernel,
        grid=(kinds,),
        in_specs=[pl.BlockSpec((1, rows, lanes), lambda i: (i, 0, 0))],
        out_specs=pl.BlockSpec((1, HEADS, WTOK * WTOK), lambda i: (i, 0, 0)),
        out_shape=jax.ShapeDtypeStruct((kinds, HEADS, WTOK * WTOK), F32),
        scratch_shapes=[pltpu.VMEM((stack, LANES), F32), pltpu.VMEM((stack, LANES), F32)],
        cost_estimate=pl.CostEstimate(
            flops=10_000_000_000, bytes_accessed=15_000_000, transcendentals=0
        ),
    )(packed)


def spread_kernel(flat_ref, main_ref, tail_ref, main_s, tail_s):
    group = LANES // TAIL
    lane = lax.broadcasted_iota(jnp.int32, (HEADS, LANES), 1)

    def body(m, _):
        tiles = []
        for r in range(group + 1):
            start = pl.multiple_of(m * (group * WTOK) + r * LANES, LANES)
            tiles.append(flat_ref[0, :, pl.ds(start, LANES)].astype(F32))
        for r in range(group):
            main, tail = tiles[r], tiles[r + 1]
            if r:
                main = jnp.where(lane >= TAIL * r, main, tail)
                main = pltpu.roll(main, LANES - TAIL * r, 1)
                tail = pltpu.roll(tail, LANES - TAIL * r, 1)
            at = pl.ds(m * group + r, HEADS, stride=WTOK)
            main_s[at, :] = main
            tail_s[at, :] = tail
        return 0

    lax.fori_loop(0, WTOK // group, body, 0)
    main_ref[0] = main_s[...].astype(BF16)
    tail_ref[0] = tail_s[:, :TAIL].astype(BF16)


def spread_whole(flat_ref, out_ref, main_s, tail_s):
    spread_kernel(
        flat_ref, out_ref.at[:, :, :LANES], out_ref.at[:, :, LANES:], main_s, tail_s
    )


def spread(table):
    kinds = table.shape[0]
    stack = HEADS * WTOK
    return pl.pallas_call(
        spread_whole,
        grid=(kinds,),
        in_specs=[pl.BlockSpec((1, HEADS, WTOK * WTOK), lambda i: (i, 0, 0))],
        out_specs=pl.BlockSpec((1, stack, WTOK), lambda i: (i, 0, 0)),
        out_shape=jax.ShapeDtypeStruct((kinds, stack, WTOK), BF16),
        scratch_shapes=[pltpu.VMEM((stack, LANES), F32), pltpu.VMEM((stack, LANES), F32)],
        cost_estimate=pl.CostEstimate(
            flops=10_000_000_000, bytes_accessed=15_000_000, transcendentals=0
        ),
    )(table)


def window_call(chunk, last, perm, frame_in, frame_cot, weight_qkv, weight_proj, bias):
    levels, height, wide, channels = frame_in.shape
    level_windows = levels // WIN_Z
    lat_windows = height // WIN_LAT
    lon_windows = perm.shape[0] // WTOK
    rows_here = lat_windows // CHUNKS
    first = chunk * rows_here
    kinds = rows_here * level_windows

    def at(step, up):
        z = lax.rem(WIN_Z * lax.rem(step, level_windows) + up, levels)
        return z, step // level_windows + first, 0, 0

    tok = (1, WIN_LAT, wide, channels)
    low = pl.BlockSpec(tok, lambda i: at(i, 1))
    high = pl.BlockSpec(tok, lambda i: at(i, 2))
    whole = lambda arr: pl.BlockSpec(arr.shape, lambda i: (0,) * arr.ndim)
    const = lambda shape: pl.BlockSpec(shape, lambda i: (0,) * len(shape))
    stack = HEADS * WTOK
    packed = stack + WTOK
    return pl.pallas_call(
        functools.partial(kernel, first, lat_windows, level_windows, lon_windows),
        grid=(kinds,),
        in_specs=[
            pl.BlockSpec(memory_space=pltpu.SMEM),
            whole(perm),
            low,
            high,
            low,
            high,
            whole(weight_qkv),
            whole(weight_proj),
            pl.BlockSpec((1, stack, WTOK), lambda i: (i + first * level_windows, 0, 0)),
        ],
        out_specs=[
            pl.BlockSpec(
                (WIN_Z, WIN_LAT, wide, channels),
                lambda i: (lax.rem(i, level_windows), i // level_windows, 0, 0),
            ),
            const((channels, 3 * channels)),
            const((channels, channels)),
            pl.BlockSpec((1, packed, LANES), lambda i: (i, 0, 0)),
        ],
        out_shape=[
            jax.ShapeDtypeStruct((levels, rows_here * WIN_LAT, wide, channels), BF16),
            jax.ShapeDtypeStruct((channels, 3 * channels), F32),
            jax.ShapeDtypeStruct((channels, channels), F32),
            jax.ShapeDtypeStruct((kinds, packed, LANES), BF16),
        ],
        scratch_shapes=[
            pltpu.VMEM((lon_windows, stack, channels), BF16),
            pltpu.VMEM((lon_windows, stack, channels), BF16),
            pltpu.VMEM((lon_windows, stack, WTOK), BF16),
            pltpu.VMEM((lon_windows, stack, WTOK), BF16),
        ],
        compiler_params=pltpu.CompilerParams(
            dimension_semantics=("arbitrary",), vmem_limit_bytes=48 * 2**20
        ),
        cost_estimate=pl.CostEstimate(
            flops=kinds * 1_500_000_000, bytes_accessed=kinds * 2_000_000, transcendentals=0
        ),
    )(
        last, perm, frame_in, frame_in, frame_cot, frame_cot, weight_qkv, weight_proj, bias
    )


def local(normed, cotangent, weight_qkv, weight_proj, bias_table):
    levels, height, breadth, channels = normed.shape
    lat_shift = WIN_LAT // 2
    lon_shift = WIN_LON // 2
    lon_windows = breadth // WIN_LON
    wide = breadth + HALO
    across = ring_permute((normed[:, :, :HALO], cotangent[:, :, :HALO]), "lon", -1)
    wide_in = jnp.concatenate([normed, across[0]], axis=2)
    wide_cot = jnp.concatenate([cotangent, across[1]], axis=2)
    upward = line_permute((wide_in[:, :lat_shift], wide_cot[:, :lat_shift]), "lat", -1)
    frame_in = jnp.concatenate([wide_in[:, lat_shift:], upward[0]], axis=1)
    frame_cot = jnp.concatenate([wide_cot[:, lat_shift:], upward[1]], axis=1)
    last = (lax.axis_index("lat") == lax.axis_size("lat") - 1).astype(jnp.int32).reshape(1)
    bias = spread(bias_table)

    rows = jnp.arange(lon_windows * WTOK, dtype=jnp.int32)
    token = rows % WTOK
    per_level = WIN_LAT * WIN_LON
    source = (
        token // per_level * (WIN_LAT * wide)
        + token % per_level // WIN_LON * wide
        + rows // WTOK * WIN_LON
        + token % WIN_LON
        + lon_shift
    )
    columns = jnp.arange(WIN_Z * WIN_LAT * wide, dtype=jnp.int32)
    perm = (source[:, None] == columns[None, :]).astype(BF16)

    gframe, gqkv, gproj, gbias = window_call(
        0, last, perm, frame_in, frame_cot, weight_qkv, weight_proj, bias
    )
    weights = jnp.concatenate([gqkv, gproj], axis=1).astype(BF16)
    packed, weights = reduce_all(gbias, weights)
    weights = weights.astype(F32)

    gwide = jnp.roll(gframe, WIN_Z // 2, axis=0)
    side = ring_permute(gwide[:, :, breadth:], "lon", 1)
    seam = jnp.concatenate(
        [gwide[:, :, :HALO] + side, gwide[:, :, HALO:breadth]], axis=2
    )
    down = line_permute(seam[:, height - lat_shift :], "lat", 1)
    input_grad = jnp.concatenate([down, seam[:, : height - lat_shift]], axis=1)

    bias_grad = unpack(packed)
    return input_grad, weights[:, : 3 * channels], weights[:, 3 * channels :], bias_grad


def solution(mesh):
    in_specs = (
        P(None, "lat", "lon", None),
        P(None, "lat", "lon", None),
        P(),
        P(),
        P("lat", None, None),
    )
    out_specs = (P(None, "lat", "lon", None), P(), P(), P("lat", None, None))
    return jax.shard_map(local, mesh=mesh, in_specs=in_specs, out_specs=out_specs, check_vma=False)
```

```python
import functools
import math

import jax
import jax.numpy as jnp
from jax import lax
from jax.experimental import pallas as pl
from jax.experimental.pallas import tpu as pltpu
from jax.sharding import PartitionSpec as P

HEADS = 6
WIN_Z = 2
WIN_LAT = 6
WIN_LON = 12
WTOK = 144
LANES = 128
TAIL = WTOK - LANES
HALO = 8
CHUNKS = 1
UNROLL = 6
LOG2E = math.log2(math.e)
F32 = jnp.float32
BF16 = jnp.bfloat16


def ring_permute(block, axis, distance):
    size = lax.axis_size(axis)
    return lax.ppermute(block, axis, [((i - distance) % size, i) for i in range(size)])


def line_permute(block, axis, distance):
    size = lax.axis_size(axis)
    route = [(i - distance, i) for i in range(size) if 0 <= i - distance < size]
    return lax.ppermute(block, axis, route)


def mm(a, b, ca=1, cb=0):
    return lax.dot_general(a, b, (((ca,), (cb,)), ((), ())), preferred_element_type=F32)


def kernel(
    first_row,
    lat_windows,
    level_windows,
    lon_windows,
    last_ref,
    perm_ref,
    xa_ref,
    xb_ref,
    ca_ref,
    cb_ref,
    wqkv_ref,
    wproj_ref,
    bias_ref,
    gframe_ref,
    gqkv_ref,
    gproj_ref,
    gbias_ref,
    qm_s,
    mm_s,
    p_s,
    ds_s,
):
    step = pl.program_id(0)
    a = lax.rem(step, level_windows)
    b = step // level_windows + first_row
    channels = wqkv_ref.shape[0]
    head_dim = channels // HEADS
    scale = head_dim ** -0.5
    half = WIN_LAT * xa_ref.shape[2]

    @pl.when(step == 0)
    def _():
        gqkv_ref[...] = jnp.zeros_like(gqkv_ref)
        gproj_ref[...] = jnp.zeros_like(gproj_ref)

    perm = perm_ref[...]
    x_raw = jnp.concatenate(
        [xa_ref[...].reshape(half, channels), xb_ref[...].reshape(half, channels)], axis=0
    )
    c_raw = jnp.concatenate(
        [ca_ref[...].reshape(half, channels), cb_ref[...].reshape(half, channels)], axis=0
    )
    x = mm(perm, x_raw).astype(BF16)
    c = mm(perm, c_raw).astype(BF16)
    proj = mm(x, wqkv_ref[...]).astype(BF16)
    mgrad = mm(c, wproj_ref[...], 1, 1).astype(BF16)

    wrap_here = a == level_windows - 1
    dead_here = (b == lat_windows - 1) & (last_ref[0] == 1)
    per_level = WTOK // WIN_Z

    def classes(shape, dim):
        token = lax.broadcasted_iota(jnp.int32, shape, dim)
        upper = token >= per_level
        inner = jnp.where(upper, token - per_level, token)
        wrapped = jnp.where(upper & wrap_here, 2, 0)
        dead = jnp.where((inner >= per_level // 2) & dead_here, 1, 0)
        return wrapped + dead

    same = classes((WTOK, WTOK), 0) == classes((WTOK, WTOK), 1)
    mask_add = jnp.where(same, 0.0, -1e30)
    lane_head = lax.broadcasted_iota(jnp.int32, (1, channels), 1) // head_dim
    zero = jnp.zeros((), BF16)

    parts = []
    for w in range(lon_windows):
        rows = slice(w * WTOK, (w + 1) * WTOK)
        parts.append(
            (
                proj[rows, :channels],
                proj[rows, channels : 2 * channels],
                proj[rows, 2 * channels :],
                mgrad[rows],
            )
        )
    mixed = [jnp.zeros((WTOK, channels), F32) for _ in range(lon_windows)]
    dq = [jnp.zeros((WTOK, channels), F32) for _ in range(lon_windows)]
    for h in range(HEADS):
        hot = (lane_head == h).astype(BF16)
        hrows = slice(h * WTOK, (h + 1) * WTOK)
        shift = bias_ref[0, hrows, :].astype(F32) * LOG2E + mask_add
        gb = None
        for w in range(lon_windows):
            q, k, v, m = parts[w]
            qm = q * hot
            mg = m * hot
            qm_s[w, hrows, :] = qm
            mm_s[w, hrows, :] = mg
            s = mm(qm, k, 1, 1) * (scale * LOG2E) + shift
            dp = mm(mg, v, 1, 1)
            e = jnp.exp2(s - jnp.max(s, axis=1, keepdims=True))
            p = e * (1.0 / jnp.sum(e, axis=1, keepdims=True))
            delta = jnp.sum(p * dp, axis=1, keepdims=True)
            ds = p * (dp - delta)
            pb = p.astype(BF16)
            dsb = ds.astype(BF16)
            p_s[w, hrows, :] = pb
            ds_s[w, hrows, :] = dsb
            gb = ds if gb is None else gb + ds
            mixed[w] = mixed[w] + mm(pb, v * hot)
            dq[w] = dq[w] + mm(dsb, k * hot)
        gb = gb.astype(BF16)
        gbias_ref[0, hrows, :] = gb[:, :LANES]
        gbias_ref[0, HEADS * WTOK :, h * TAIL : (h + 1) * TAIL] = gb[:, LANES:]
    cols = []
    for w in range(lon_windows):
        dk = mm(ds_s[w], qm_s[w], 0, 0) * scale
        dv = mm(p_s[w], mm_s[w], 0, 0)
        cols.append(
            jnp.concatenate(
                [(dq[w] * scale).astype(BF16), dk.astype(BF16), dv.astype(BF16)], axis=1
            )
        )
    cols = jnp.concatenate(cols, axis=0)
    mixed_b = jnp.concatenate([t.astype(BF16) for t in mixed], axis=0)
    gproj_ref[...] += mm(mixed_b, c, 0, 0)
    gqkv_ref[...] += mm(x, cols, 0, 0)
    gin = mm(cols, wqkv_ref[...], 1, 1).astype(BF16)
    gout = mm(perm, gin, 0, 0).astype(BF16)
    gframe_ref[...] = gout.reshape(gframe_ref.shape)


def reduce_kernel(
    n, lats, gb_ref, wg_ref, out_ref, wout_ref, pair_s, send_s, recv_s, w1_s, w2_s,
    pair_sem, cross_sem, back_sem, fwd_sem, w1_sem, w2_sem, w3_sem,
):
    chips = n // 2
    me = lax.axis_index("lon")
    lat = lax.axis_index("lat")
    core = lax.rem(me, 2)
    chip = me // 2
    other = 1 - core
    partner = chip * 2 + other
    types = gb_ref.shape[0]
    share = types // n

    def piece(which, where):
        return pl.ds((which * chips + where) * share, share)

    def copy(src, dst, sems, out_at, in_at, device):
        return pltpu.make_async_remote_copy(
            src_ref=src,
            dst_ref=dst,
            send_sem=sems.at[0, out_at],
            recv_sem=sems.at[1, in_at],
            device_id=device,
            device_id_type=pl.DeviceIdType.MESH,
        )

    barrier = pltpu.get_barrier_semaphore()
    for o in range(1, n):
        pl.semaphore_signal(
            barrier, inc=1, device_id={"lon": lax.rem(me + o, n)},
            device_id_type=pl.DeviceIdType.MESH,
        )
    for o in range(1, lats):
        pl.semaphore_signal(
            barrier, inc=1, device_id={"lat": lax.rem(lat + o, lats)},
            device_id_type=pl.DeviceIdType.MESH,
        )
    pl.semaphore_wait(barrier, n + lats - 2)

    order = [(o, lax.rem(chip + o, chips)) for o in list(range(1, chips)) + [0]]
    sends = []
    first = []
    for o in range(1, n):
        p = lax.rem(me + o, n)
        cp = copy(wg_ref.at[p], w1_s.at[me], w1_sem, p, me, {"lon": p})
        cp.start()
        sends.append(cp)
    for o, j in order:
        cp = copy(gb_ref.at[piece(other, j)], pair_s.at[o], pair_sem, o, o, {"lon": partner})
        cp.start()
        first.append(cp)
    sends += first

    w1_s[pl.ds(me, 1)] = wg_ref[pl.ds(me, 1)]
    for o in range(1, n):
        p = lax.rem(me + o, n)
        copy(wg_ref.at[p], w1_s.at[p], w1_sem, p, p, {"lon": p}).wait_recv()
    w2_s[pl.ds(lat, 1)] = jnp.sum(w1_s[...].astype(F32), axis=0, keepdims=True).astype(BF16)
    for o in range(1, lats):
        p = lax.rem(lat + o, lats)
        cp = copy(w2_s.at[lat], w2_s.at[lat], w2_sem, p, lat, {"lat": p})
        cp.start()
        sends.append(cp)

    for cp, (o, j) in zip(first, order):
        cp.wait_recv()

        def add(i, _, o=o, j=j):
            mine = gb_ref[(core * chips + j) * share + i].astype(F32)
            total = (mine + pair_s[o, i].astype(F32)).astype(BF16)
            if o:
                send_s[o, i] = total
            else:
                recv_s[chip, i] = total
            return 0

        lax.fori_loop(0, share, add, 0)
        if o:
            cp2 = copy(
                send_s.at[o], recv_s.at[chip], cross_sem, o, chip, {"lon": j * 2 + core}
            )
            cp2.start()
            sends.append(cp2)

    for o in range(1, lats):
        p = lax.rem(lat + o, lats)
        copy(w2_s.at[p], w2_s.at[p], w2_sem, p, p, {"lat": p}).wait_recv()
    wout_ref[pl.ds(me, 1)] = jnp.sum(w2_s[...].astype(F32), axis=0, keepdims=True).astype(BF16)
    for o in range(1, n):
        p = lax.rem(me + o, n)
        cp = copy(wout_ref.at[me], wout_ref.at[me], w3_sem, p, me, {"lon": p})
        cp.start()
        sends.append(cp)

    for o in range(1, chips):
        j = lax.rem(chip + o, chips)
        copy(send_s.at[o], recv_s.at[j], cross_sem, o, j, {"lon": j * 2 + core}).wait_recv()

    def total(i, _):
        acc = recv_s[0, i].astype(F32)
        for j in range(1, chips):
            acc = acc + recv_s[j, i].astype(F32)
        out_ref[(core * chips + chip) * share + i] = acc.astype(BF16)
        return 0

    lax.fori_loop(0, share, total, 0)
    own = out_ref.at[piece(core, chip)]
    for o in range(1, chips):
        j = lax.rem(chip + o, chips)
        cp = copy(own, own, back_sem, j, chip, {"lon": j * 2 + core})
        cp.start()
        sends.append(cp)
    cp = copy(own, own, fwd_sem, chip, chip, {"lon": partner})
    cp.start()
    sends.append(cp)
    for o in range(1, chips):
        j = lax.rem(chip + o, chips)
        part = out_ref.at[piece(core, j)]
        copy(part, part, back_sem, j, j, {"lon": j * 2 + core}).wait_recv()
        cp = copy(part, part, fwd_sem, j, j, {"lon": partner})
        cp.start()
        sends.append(cp)
    for j in range(chips):
        part = out_ref.at[piece(other, j)]
        copy(part, part, fwd_sem, j, j, {"lon": partner}).wait_recv()
    for o in range(1, n):
        p = lax.rem(me + o, n)
        copy(wout_ref.at[p], wout_ref.at[p], w3_sem, p, p, {"lon": p}).wait_recv()
    for cp in sends:
        cp.wait_send()


def reduce_all(gbias, weights):
    n, lats = lax.axis_size("lon"), lax.axis_size("lat")
    chips = n // 2
    types, packed, lanes = gbias.shape
    rows, width = weights.shape
    share = types // n
    weights = weights.reshape(n, rows // n, width)
    vm = pl.BlockSpec(memory_space=pltpu.VMEM)
    sem = lambda k: pltpu.SemaphoreType.DMA((2, k))
    block = pltpu.VMEM((chips, share, packed, lanes), BF16)
    out, wout = pl.pallas_call(
        functools.partial(reduce_kernel, n, lats),
        in_specs=[vm, vm],
        out_specs=[vm, vm],
        out_shape=[
            jax.ShapeDtypeStruct(gbias.shape, BF16),
            jax.ShapeDtypeStruct(weights.shape, BF16),
        ],
        scratch_shapes=[
            block,
            block,
            block,
            pltpu.VMEM((n, rows // n, width), BF16),
            pltpu.VMEM((lats, rows // n, width), BF16),
            sem(chips),
            sem(chips),
            sem(chips),
            sem(chips),
            sem(n),
            sem(lats),
            sem(n),
        ],
        compiler_params=pltpu.CompilerParams(
            collective_id=0, has_side_effects=True, vmem_limit_bytes=40 * 2**20
        ),
        cost_estimate=pl.CostEstimate(
            flops=30_000_000_000, bytes_accessed=60_000_000, transcendentals=0
        ),
    )(gbias, weights)
    return out, wout.reshape(rows, width)


def unpack_kernel(packed_ref, out_ref, main_s, tail_s):
    stack = HEADS * WTOK
    main_s[...] = packed_ref[0, :stack].astype(F32)
    tails = packed_ref[0, stack:].astype(F32)
    for h in range(HEADS):
        turned = tails if h == 0 else pltpu.roll(tails, LANES - h * TAIL, 1)
        tail_s[h * WTOK : (h + 1) * WTOK] = turned
    group = LANES // TAIL
    lane = lax.broadcasted_iota(jnp.int32, (HEADS, LANES), 1)

    def body(m, _):
        before_main = before_tail = None
        for r in range(group + 1):
            tile = None
            if r < group:
                at = pl.ds(m * group + r, HEADS, stride=WTOK)
                here_main, here_tail = main_s[at, :], tail_s[at, :]
                if r:
                    here_main = pltpu.roll(here_main, TAIL * r, 1)
                    here_tail = pltpu.roll(here_tail, TAIL * r, 1)
                tile = here_main
            if r:
                ended = before_tail
                if r > 1:
                    ended = jnp.where(lane < TAIL * (r - 1), before_main, before_tail)
                tile = ended if r == group else jnp.where(lane < TAIL * r, ended, tile)
            start = pl.multiple_of(m * (group * WTOK) + r * LANES, LANES)
            out_ref[0, :, pl.ds(start, LANES)] = tile
            if r < group:
                before_main, before_tail = here_main, here_tail
        return 0

    def several(i, _):
        for u in range(UNROLL):
            body(i * UNROLL + u, 0)
        return 0

    lax.fori_loop(0, WTOK // group // UNROLL, several, 0)


def unpack(packed):
    kinds, rows, lanes = packed.shape
    stack = HEADS * WTOK
    return pl.pallas_call(
        unpack_kernel,
        grid=(kinds,),
        in_specs=[pl.BlockSpec((1, rows, lanes), lambda i: (i, 0, 0))],
        out_specs=pl.BlockSpec((1, HEADS, WTOK * WTOK), lambda i: (i, 0, 0)),
        out_shape=jax.ShapeDtypeStruct((kinds, HEADS, WTOK * WTOK), F32),
        scratch_shapes=[pltpu.VMEM((stack, LANES), F32), pltpu.VMEM((stack, LANES), F32)],
        cost_estimate=pl.CostEstimate(
            flops=10_000_000_000, bytes_accessed=15_000_000, transcendentals=0
        ),
    )(packed)


def window_call(chunk, last, perm, frame_in, frame_cot, weight_qkv, weight_proj, bias):
    levels, height, wide, channels = frame_in.shape
    level_windows = levels // WIN_Z
    lat_windows = height // WIN_LAT
    lon_windows = perm.shape[0] // WTOK
    rows_here = lat_windows // CHUNKS
    first = chunk * rows_here
    kinds = rows_here * level_windows

    def at(step, up):
        z = lax.rem(WIN_Z * lax.rem(step, level_windows) + up, levels)
        return z, step // level_windows + first, 0, 0

    tok = (1, WIN_LAT, wide, channels)
    low = pl.BlockSpec(tok, lambda i: at(i, 1))
    high = pl.BlockSpec(tok, lambda i: at(i, 2))
    whole = lambda arr: pl.BlockSpec(arr.shape, lambda i: (0,) * arr.ndim)
    const = lambda shape: pl.BlockSpec(shape, lambda i: (0,) * len(shape))
    stack = HEADS * WTOK
    packed = stack + WTOK
    return pl.pallas_call(
        functools.partial(kernel, first, lat_windows, level_windows, lon_windows),
        grid=(kinds,),
        in_specs=[
            pl.BlockSpec(memory_space=pltpu.SMEM),
            whole(perm),
            low,
            high,
            low,
            high,
            whole(weight_qkv),
            whole(weight_proj),
            pl.BlockSpec((1, stack, WTOK), lambda i: (i + first * level_windows, 0, 0)),
        ],
        out_specs=[
            pl.BlockSpec(
                (WIN_Z, WIN_LAT, wide, channels),
                lambda i: (lax.rem(i, level_windows), i // level_windows, 0, 0),
            ),
            const((channels, 3 * channels)),
            const((channels, channels)),
            pl.BlockSpec((1, packed, LANES), lambda i: (i, 0, 0)),
        ],
        out_shape=[
            jax.ShapeDtypeStruct((levels, rows_here * WIN_LAT, wide, channels), BF16),
            jax.ShapeDtypeStruct((channels, 3 * channels), F32),
            jax.ShapeDtypeStruct((channels, channels), F32),
            jax.ShapeDtypeStruct((kinds, packed, LANES), BF16),
        ],
        scratch_shapes=[
            pltpu.VMEM((lon_windows, stack, channels), BF16),
            pltpu.VMEM((lon_windows, stack, channels), BF16),
            pltpu.VMEM((lon_windows, stack, WTOK), BF16),
            pltpu.VMEM((lon_windows, stack, WTOK), BF16),
        ],
        compiler_params=pltpu.CompilerParams(
            dimension_semantics=("arbitrary",), vmem_limit_bytes=48 * 2**20
        ),
        cost_estimate=pl.CostEstimate(
            flops=kinds * 1_500_000_000, bytes_accessed=kinds * 2_000_000, transcendentals=0
        ),
    )(
        last, perm, frame_in, frame_in, frame_cot, frame_cot, weight_qkv, weight_proj, bias
    )


def local(normed, cotangent, weight_qkv, weight_proj, bias_table):
    levels, height, breadth, channels = normed.shape
    lat_shift = WIN_LAT // 2
    lon_shift = WIN_LON // 2
    lon_windows = breadth // WIN_LON
    wide = breadth + HALO
    across = ring_permute((normed[:, :, :HALO], cotangent[:, :, :HALO]), "lon", -1)
    wide_in = jnp.concatenate([normed, across[0]], axis=2)
    wide_cot = jnp.concatenate([cotangent, across[1]], axis=2)
    upward = line_permute((wide_in[:, :lat_shift], wide_cot[:, :lat_shift]), "lat", -1)
    frame_in = jnp.concatenate([wide_in[:, lat_shift:], upward[0]], axis=1)
    frame_cot = jnp.concatenate([wide_cot[:, lat_shift:], upward[1]], axis=1)
    last = (lax.axis_index("lat") == lax.axis_size("lat") - 1).astype(jnp.int32).reshape(1)
    bias = bias_table.reshape(bias_table.shape[0], HEADS * WTOK, WTOK)

    rows = jnp.arange(lon_windows * WTOK, dtype=jnp.int32)
    token = rows % WTOK
    per_level = WIN_LAT * WIN_LON
    source = (
        token // per_level * (WIN_LAT * wide)
        + token % per_level // WIN_LON * wide
        + rows // WTOK * WIN_LON
        + token % WIN_LON
        + lon_shift
    )
    columns = jnp.arange(WIN_Z * WIN_LAT * wide, dtype=jnp.int32)
    perm = (source[:, None] == columns[None, :]).astype(BF16)

    gframe, gqkv, gproj, gbias = window_call(
        0, last, perm, frame_in, frame_cot, weight_qkv, weight_proj, bias
    )
    weights = jnp.concatenate([gqkv, gproj], axis=1).astype(BF16)
    packed, weights = reduce_all(gbias, weights)
    weights = weights.astype(F32)

    gwide = jnp.roll(gframe, WIN_Z // 2, axis=0)
    side = ring_permute(gwide[:, :, breadth:], "lon", 1)
    seam = jnp.concatenate(
        [gwide[:, :, :HALO] + side, gwide[:, :, HALO:breadth]], axis=2
    )
    down = line_permute(seam[:, height - lat_shift :], "lat", 1)
    input_grad = jnp.concatenate([down, seam[:, : height - lat_shift]], axis=1)

    bias_grad = unpack(packed)
    return input_grad, weights[:, : 3 * channels], weights[:, 3 * channels :], bias_grad


def solution(mesh):
    in_specs = (
        P(None, "lat", "lon", None),
        P(None, "lat", "lon", None),
        P(),
        P(),
        P("lat", None, None),
    )
    out_specs = (P(None, "lat", "lon", None), P(), P(), P("lat", None, None))
    return jax.shard_map(local, mesh=mesh, in_specs=in_specs, out_specs=out_specs, check_vma=False)
```
